128 devices in a mesh: lat: 8 (over y, core), lon: 16 (over z, x).
Axes of the slice: x: 4, y: 4, z: 4, core: 2. Of those that a mesh axis runs over, the one named last changes fastest.
Arguments:
- coarse: bfloat16 [122880, 1104], P(('lat', 'lon')), may hold values from -6 to 6
- w_mix: bfloat16 [69, 64], replicated, may hold values from -0.75 to 0.75
- interp: bfloat16 [16, 256], replicated, may hold values from -1.5 to 1.5
- kernel: bfloat16 [3, 3, 64, 64], replicated, may hold values from -0.25 to 0.25
- bias: float32 [64], replicated, may hold values from -3 to 3
- block_ids: int32 [128, 144], replicated, may hold values from 0 to 122879, as said below
- valid: int32 [128, 144], replicated, may hold values from 0 to 1, as said below
Outputs:
- fine_out: bfloat16 [64, 2304, 2048], P(None, 'lat', 'lon')
The draws below stay inside these ranges and needn't reach their ends.
Inputs may be any that keep to these rules, and one draw needn't show every extreme that they name: `block_ids`: the coarse grid has 192 block rows and 640 block columns, held block-cyclically: block (r, c) is row ((r mod 8) * 16 + c mod 16) * 960 + (r div 8) * 40 + c div 16 of coarse. Slot p of tile t holds block (r0 + (t div 16) * 18 + p div 8, (c0 + (t mod 16) * 8 + p mod 8) mod (640)), with offsets r0 and c0 common to all tiles. Among the valid slots of one tile at most 3 name blocks of one device, and in every tile exactly 3 valid slots name blocks of some one device. Every tile has 3 or more valid slots.
All inputs are finite; a program needn't handle non-finite values.
Results may differ from the reference program's by a relative error of at most 0.0055.
Values may be sent and summed in bfloat16 or wider, within the bound.
No kernel may reach another device: no remote copies, remote signals or barrier semaphores. Data moves between devices by JAX's collectives and lax.ppermute only.
A program may use at most 192 MiB of HBM per device.

```python
import jax
import jax.numpy as jnp
from jax import lax

C_IN = 69
C = 64
CB_ROWS = 24
CB_COLS = 40
PR = 18
PC = 8
CB_DEV = 960
PATCHES = 144
TH = 288
TW = 128
TILES = 128
BLOCKS = 122880
N_LAT = 8
N_LON = 16
DEVICES = 128


def route_table(key):
    base = jax.random.fold_in(key, 11)
    keys = jax.random.split(base, 6)
    grid_cols = N_LON * CB_COLS
    row_start = jax.random.randint(keys[0], (), 0, N_LAT * (CB_ROWS - PR) + 1)
    col_start = jax.random.randint(keys[1], (), 0, grid_cols)
    tiles = jnp.arange(DEVICES, dtype=jnp.int32)
    tile_lat = tiles // N_LON
    tile_lon = tiles % N_LON
    slots = jnp.arange(PATCHES, dtype=jnp.int32)
    patch_row = slots // PC
    patch_col = slots % PC
    rows = row_start + tile_lat[:, None] * PR + patch_row[None, :]
    cols = (col_start + tile_lon[:, None] * PC + patch_col[None, :]) % grid_cols
    owner = rows % N_LAT * N_LON + cols % N_LON
    local = rows // N_LAT * CB_COLS + cols // N_LON
    ids = (owner * CB_DEV + local).astype(jnp.int32)
    slope_row = jax.random.randint(keys[2], (DEVICES, 1), -3, 4)
    slope_col = jax.random.randint(keys[3], (DEVICES, 1), -3, 4)
    rough = jax.random.randint(keys[4], (DEVICES, PATCHES), 0, 4)
    cut = jax.random.randint(keys[5], (DEVICES, 1), -2 * PC, PC // 2 + 1)
    score = slope_row * (patch_row[None, :] - PR // 2) + slope_col * (patch_col[None, :] - PC // 2) + rough
    forced = owner == owner[:, :1]
    live = ((score >= cut) | forced).astype(jnp.int32)
    return (ids, live)


def draw_block_ids(key, part):
    return route_table(key)[0]


def draw_valid(key, part):
    return route_table(key)[1]


def shard_levels(own_key, shape, shards, least, largest):
    def one(position, shards_of):
        heights = jax.random.uniform(jax.random.fold_in(jax.random.fold_in(own_key, 6), position), (shards_of,), jnp.float32, least / len(shards), largest / len(shards))
        return jnp.repeat(jnp.exp(heights), shape[position] // shards_of).reshape((-1,) + (1,) * (len(shape) - position - 1))

    loudness = one(*shards[0])
    for cut in shards[1:]:
        loudness = loudness * one(*cut)
    return loudness


def gaussian(stream_key, extent, scale, bound, cuts=(), kind=jnp.bfloat16):
    entries = jax.random.normal(stream_key, extent, jnp.float32) * scale
    if len(cuts) > 0:
        entries = shard_levels(stream_key, extent, cuts, -0.22, 0.18) * entries
    return jnp.clip(entries, min=-bound, max=bound).astype(kind)


def setup_inputs(seed: int = 0) -> dict:
    arg_keys = jax.random.split(jax.random.key(seed), 8)
    return {
        "coarse": gaussian(arg_keys[0], (BLOCKS, 16 * C_IN), 1.0, 6.0, ((0, 128),)),
        "w_mix": gaussian(arg_keys[1], (C_IN, C), C_IN ** -0.5, 0.75),
        "interp": gaussian(arg_keys[2], (16, 256), 16 ** -0.5, 1.5),
        "kernel": gaussian(arg_keys[3], (3, 3, C, C), (9 * C) ** -0.5, 0.25),
        "bias": gaussian(arg_keys[4], (C,), 0.5, 3.0, (), jnp.float32),
        "block_ids": draw_block_ids(jax.random.fold_in(arg_keys[7], 71), 0),
        "valid": draw_valid(jax.random.fold_in(arg_keys[7], 71), 0),
    }


def mix_rows(rows, w_mix):
    count = rows.shape[0]
    flat = rows.reshape(count * 16, C_IN)
    mapped = jnp.dot(flat, w_mix, preferred_element_type=jnp.float32).astype(jnp.bfloat16)
    return mapped.reshape(count, 16, C)


def reference(coarse, w_mix, interp, kernel, bias, block_ids, valid):
    mixed = mix_rows(coarse, w_mix)
    interp_f = interp.astype(jnp.float32)

    def tile_image(tile):
        picked = mixed[block_ids[tile]].astype(jnp.float32)
        fine = jnp.einsum('pkc,kf->pcf', picked, interp_f).astype(jnp.bfloat16)
        fine = fine * valid[tile][:, None, None].astype(jnp.bfloat16)
        fine = fine.reshape(PR, PC, C, 16, 16).transpose(2, 0, 3, 1, 4)
        return fine.reshape(C, TH, TW)

    tiles = lax.map(tile_image, jnp.arange(TILES, dtype=jnp.int32))
    field = tiles.reshape(N_LAT, N_LON, C, TH, TW).transpose(2, 0, 3, 1, 4).reshape(C, N_LAT * TH, N_LON * TW)
    land = valid.astype(jnp.float32).reshape(N_LAT, N_LON, PR, PC)
    land = jnp.repeat(jnp.repeat(land, 16, axis=2), 16, axis=3)
    land = land.transpose(0, 2, 1, 3).reshape(N_LAT * TH, N_LON * TW)
    padded = jnp.pad(field, ((0, 0), (1, 1), (1, 1)))
    kernel_f = kernel.astype(jnp.float32)
    width = N_LON * TW

    def band(index):
        rows = lax.dynamic_slice_in_dim(padded, (index * TH).astype(jnp.int32), TH + 2, 1).astype(jnp.float32)
        total = jnp.zeros((C, TH, width), jnp.float32)
        for tap_row in range(3):
            for tap_col in range(3):
                total = total + jnp.einsum('oc,chw->ohw', kernel_f[tap_row, tap_col], rows[:, tap_row:tap_row + TH, tap_col:tap_col + width])
        mask_rows = lax.dynamic_slice_in_dim(land, (index * TH).astype(jnp.int32), TH, 0)
        return ((total + bias[:, None, None]) * mask_rows[None]).astype(jnp.bfloat16)

    bands = lax.map(band, jnp.arange(N_LAT, dtype=jnp.int32))
    return bands.transpose(1, 0, 2, 3).reshape(C, N_LAT * TH, width)
```

```python
import jax
import jax.numpy as jnp
from jax import lax
from jax.experimental import pallas as pl
from jax.experimental.pallas import tpu as pltpu
from jax.sharding import PartitionSpec as P

PR = 18
PC = 8
CELLS = 16
WR = PR + 2
WC = PC + 2
MOST = 3
CB_ROWS = 24
CB_COLS = 40
HELD_ROWS = 20
C_IN = 69
C = 64
GRID_COLS = 640


def pack_body(ids_ref, coarse_ref, w_ref, out_ref, raw, weights, mixed, sems):
    n_lat, n_lon = 8, 16
    a = lax.axis_index("lat")
    b = lax.axis_index("lon")
    first = ids_ref[0, 0]
    owner = first // (CB_ROWS * CB_COLS)
    local = first % (CB_ROWS * CB_COLS)
    r0 = (local // CB_COLS) * n_lat + owner // n_lon
    c0 = (local % CB_COLS) * n_lon + owner % n_lon
    low = jnp.clip((r0 + 7) // 8 - 1, 0, CB_ROWS - HELD_ROWS)
    c_first = c0 - 1 + (b - c0 + 1 + 16 * CB_COLS) % n_lon
    lc_first = ((c_first + GRID_COLS) % GRID_COLS) // n_lon
    tile0 = lc_first // 8
    tile1 = (tile0 + 1) % (CB_COLS // 8)
    copies = []
    for slot, tile in ((0, tile0), (1, tile1)):
        copy = pltpu.make_async_copy(
            coarse_ref.at[pl.ds(low, HELD_ROWS), pl.ds(pl.multiple_of(tile * 8, 8), 8), :],
            raw.at[slot],
            sems.at[slot],
        )
        copy.start()
        copies.append(copy)
    w = w_ref[...].astype(jnp.float32)
    weights[...] = jnp.zeros_like(weights)
    for j in range(8):
        weights[j, 10 * j : 10 * j + C_IN, 0:C] = w
        weights[j, 10 * j + C_IN : 10 * j + 2 * C_IN, C : 2 * C] = w
    for copy in copies:
        copy.wait()
    count = 2 * HELD_ROWS * 8
    for j in range(8):
        width = min(256, CELLS * C_IN - 128 * j)
        rows = raw[:, :, :, 128 * j : 128 * j + width].reshape(count, width)
        part = jnp.dot(
            rows, weights[j, 0:width, :].astype(jnp.bfloat16), preferred_element_type=jnp.float32
        )
        mixed[pl.ds(j, count, stride=8), :] = part
    starts = []
    for i in range(n_lat):
        top = r0 + PR * i - 1
        r_first = top + (a - top + 512) % n_lat
        lr = (r_first + 8) // 8 - 1 - low
        for m in range(MOST):
            starts.append(jnp.clip(lr + m, 0, HELD_ROWS - 1) * 8)

    def one_column(j, carry):
        left = c0 + PC * j - 1
        d = (b - left + 16 * CB_COLS) % n_lon
        n = (left + d - c_first) // n_lon
        pos = jnp.minimum(lc_first % 8 + n, 15)
        base = (pos // 8) * (HELD_ROWS * 8) + pos % 8
        for i in range(n_lat):
            for m in range(MOST):
                at = (base + starts[i * MOST + m]) * 8
                block = mixed[pl.ds(pl.multiple_of(at, 8), 8), :]
                out_ref[(i * n_lon + j) * MOST + m] = block.astype(jnp.bfloat16)
        return carry

    lax.fori_loop(0, n_lon, one_column, 0)


def pack(block_ids, coarse, w_mix):
    return pl.pallas_call(
        pack_body,
        out_shape=jax.ShapeDtypeStruct((128 * MOST, 8, 128), jnp.bfloat16),
        grid=(1,),
        in_specs=[
            pl.BlockSpec((8, 128), lambda g: (0, 0), memory_space=pltpu.SMEM),
            pl.BlockSpec(memory_space=pl.ANY),
            pl.BlockSpec((C_IN, C), lambda g: (0, 0)),
        ],
        out_specs=pl.BlockSpec((128 * MOST, 8, 128), lambda g: (0, 0, 0)),
        scratch_shapes=[
            pltpu.VMEM((2, HELD_ROWS, 8, CELLS * C_IN), jnp.bfloat16),
            pltpu.VMEM((8, 256, 2 * C), jnp.float32),
            pltpu.VMEM((2 * HELD_ROWS * 8 * 8, 128), jnp.float32),
            pltpu.SemaphoreType.DMA((2,)),
        ],
        name="pack",
    )(block_ids, coarse.reshape(CB_ROWS, CB_COLS, CELLS * C_IN), w_mix)


def fine_body(where_ref, inc_ref, spread_ref, taps_ref, bias_ref, land_ref, out_ref, cells, cells_t, field):
    step = pl.program_id(0)

    @pl.when(step == 0)
    def _():
        lane = lax.broadcasted_iota(jnp.int32, (8, 128), 1)
        lower = lane < C

        def pair_of_rows(q, carry):
            for col in range(WC):
                got = []
                for half in range(2):
                    at = where_ref[(2 * q + half) * WC + col]
                    block = inc_ref[jnp.maximum(at, 0)].astype(jnp.float32)
                    got.append(jnp.where(at >= 0, block, 0.0))
                u, v = got
                cells[8 * col : 8 * col + 8, :] = jnp.where(lower, u, pltpu.roll(v, C, 1))
                cells[8 * (WC + col) : 8 * (WC + col) + 8, :] = jnp.where(lower, pltpu.roll(u, C, 1), v)
            cells_t[pl.ds(pl.multiple_of(q * 128, 128), 128), :] = cells[...].T.astype(jnp.bfloat16)
            return carry

        cells[8 * 2 * WC :, :] = jnp.zeros((256 - 16 * WC, 128), jnp.float32)
        lax.fori_loop(0, WR // 2, pair_of_rows, 0)

        def upsample(n, carry):
            right = jnp.concatenate([spread_ref[2 * n], spread_ref[2 * n + 1]], axis=1)
            fine = jnp.dot(
                cells_t[:, 0 : CELLS * WC], right, preferred_element_type=jnp.float32
            ).astype(jnp.bfloat16)
            tap = n // 8
            row = 2 * (n % 8)
            field[tap, :, row] = fine[:, 0:128].reshape(WR, C, 128)
            field[tap, :, row + 1] = fine[:, 128:256].reshape(WR, C, 128)
            return carry

        lax.fori_loop(0, 24, upsample, 0)

    sub = lax.broadcasted_iota(jnp.int32, (32, 8, 128), 1)
    land = land_ref[pl.ds(step, 1), :]
    even = []
    odd = []
    for h in range(2):
        quads = []
        for q in range(2):
            blocks = []
            for tap in range(3):
                for rr in range(6):
                    row = 15 + 4 * (2 * h + q) + rr
                    blocks.append(field[tap, step + row // 16, row % 16])
            quads.append(jnp.concatenate(blocks, axis=0))
        right = jnp.concatenate(quads, axis=1)
        total = jnp.dot(taps_ref[...], right, preferred_element_type=jnp.float32)
        left = ((total[:, 0:128] + bias_ref[...]) * land).reshape(32, 8, 128)
        other = ((total[:, 128:256] + bias_ref[...]) * land).reshape(32, 8, 128)
        even.append(jnp.where(sub < 4, left, pltpu.roll(other, 4, 1)))
        odd.append(jnp.where(sub < 4, pltpu.roll(left, 4, 1), other))
    out_ref[:, 0] = jnp.concatenate(even, axis=1).astype(jnp.bfloat16)
    out_ref[:, 1] = jnp.concatenate(odd, axis=1).astype(jnp.bfloat16)


def fine(where, incoming, spread, taps, bias_rows, land):
    return pl.pallas_call(
        fine_body,
        out_shape=jax.ShapeDtypeStruct((C // 2, 2, PR * 16, 128), jnp.bfloat16),
        grid=(PR,),
        in_specs=[
            pl.BlockSpec(memory_space=pltpu.SMEM),
            pl.BlockSpec((128 * MOST, 8, 128), lambda g: (0, 0, 0), pipeline_mode=pl.Buffered(1)),
            pl.BlockSpec((48, CELLS * WC, 128), lambda g: (0, 0, 0), pipeline_mode=pl.Buffered(1)),
            pl.BlockSpec((4 * C, 18 * C), lambda g: (0, 0), pipeline_mode=pl.Buffered(1)),
            pl.BlockSpec((4 * C, 128), lambda g: (0, 0), pipeline_mode=pl.Buffered(1)),
            pl.BlockSpec((PR, 128), lambda g: (0, 0), pipeline_mode=pl.Buffered(1)),
        ],
        out_specs=pl.BlockSpec((C // 2, 2, 16, 128), lambda g: (0, 0, g, 0)),
        scratch_shapes=[
            pltpu.VMEM((256, 128), jnp.float32),
            pltpu.VMEM((WR * C, 256), jnp.bfloat16),
            pltpu.VMEM((3, WR, 16, C, 128), jnp.bfloat16),
        ],
        name="fine",
    )(where, incoming, spread, taps, bias_rows, land)


def spread_of(interp):
    cells = interp.reshape(8, 2, 16, 16).transpose(2, 1, 0, 3)
    wide = jnp.tile(cells, (1, 1, 1, WC))
    shifted = jnp.stack([wide[..., 15 + tap : 143 + tap] for tap in range(3)])
    tap = jnp.arange(3)[:, None, None]
    column = (jnp.arange(128)[None, None, :] + tap + 15) // 16
    same = column == jnp.arange(WC)[None, :, None]
    full = jnp.where(same[:, None, None, :, None, :], shifted[:, :, :, None], 0)
    return full.reshape(48, CELLS * WC, 128).astype(jnp.bfloat16)


def taps_of(kernel):
    by = kernel.transpose(2, 1, 0, 3)
    rows = [jnp.pad(by, ((0, 0), (0, 0), (r, 3 - r), (0, 0))) for r in range(4)]
    return jnp.stack(rows, axis=1).reshape(4 * C, 18 * C)


def per_device(coarse, w_mix, interp, kernel, bias, block_ids, valid):
    n_lat, n_lon = 8, 16
    i = lax.axis_index("lat")
    j = lax.axis_index("lon")
    outgoing = pack(block_ids, coarse, w_mix)
    incoming = lax.all_to_all(outgoing, ("lat", "lon"), split_axis=0, concat_axis=0, tiled=True)
    first = block_ids[0, 0]
    owner = first // (CB_ROWS * CB_COLS)
    local = first % (CB_ROWS * CB_COLS)
    r0 = (local // CB_COLS) * n_lat + owner // n_lon
    c0 = (local % CB_COLS) * n_lon + owner % n_lon
    grid = valid.reshape(n_lat, n_lon, PR, PC).transpose(0, 2, 1, 3).reshape(n_lat * PR, n_lon * PC)
    window = lax.dynamic_slice(jnp.pad(grid, 1), (i * PR, j * PC), (WR, WC))
    row = jnp.arange(WR)[:, None]
    col = jnp.arange(WC)[None, :]
    source = (r0 + PR * i - 1 + row + 8) % n_lat * n_lon + (c0 + PC * j - 1 + col + 16) % n_lon
    where = jnp.where(window > 0, source * MOST + row // 8, -1).reshape(WR * WC).astype(jnp.int32)
    own = window[1:-1, 1:-1].astype(jnp.float32)
    land = jnp.repeat(own, 16, axis=1)
    bias_rows = jnp.broadcast_to(jnp.repeat(bias, 4)[:, None], (4 * C, 128))
    out = fine(where, incoming, spread_of(interp), taps_of(kernel), bias_rows, land)
    return out.reshape(C, PR * 16, 128)


def solution(mesh):
    placed = (P(("lat", "lon"), None), P(), P(), P(), P(), P(), P())
    return jax.shard_map(
        per_device, mesh=mesh, in_specs=placed, out_specs=P(None, "lat", "lon"), check_vma=False
    )
```

```python
import jax
import jax.numpy as jnp
from jax import lax
from jax.experimental import pallas as pl
from jax.experimental.pallas import tpu as pltpu
from jax.sharding import PartitionSpec as P

PR = 18
PC = 8
CELLS = 16
WR = PR + 2
WC = PC + 2
MOST = 3
CB_ROWS = 24
CB_COLS = 40
HELD_ROWS = 20
C_IN = 69
C = 64
GRID_COLS = 640


def pack_body(ids_ref, coarse_ref, w_ref, out_ref, raw, weights, mixed, sems):
    n_lat, n_lon = 8, 16
    a = lax.axis_index("lat")
    b = lax.axis_index("lon")
    first = ids_ref[0, 0]
    owner = first // (CB_ROWS * CB_COLS)
    local = first % (CB_ROWS * CB_COLS)
    r0 = (local // CB_COLS) * n_lat + owner // n_lon
    c0 = (local % CB_COLS) * n_lon + owner % n_lon
    low = jnp.clip((r0 + 7) // 8 - 1, 0, CB_ROWS - HELD_ROWS)
    c_first = c0 - 1 + (b - c0 + 1 + 16 * CB_COLS) % n_lon
    lc_first = ((c_first + GRID_COLS) % GRID_COLS) // n_lon
    tile0 = lc_first // 8
    tile1 = (tile0 + 1) % (CB_COLS // 8)
    copies = []
    for slot, tile in ((0, tile0), (1, tile1)):
        copy = pltpu.make_async_copy(
            coarse_ref.at[pl.ds(low, HELD_ROWS), pl.ds(pl.multiple_of(tile * 8, 8), 8), :],
            raw.at[slot],
            sems.at[slot],
        )
        copy.start()
        copies.append(copy)
    w = w_ref[...].astype(jnp.float32).T
    weights[...] = jnp.zeros_like(weights)
    for j in range(8):
        weights[j, 10 * j : 10 * j + C_IN, 0:C] = w
        weights[j, 10 * j + C_IN : 10 * j + 2 * C_IN, C : 2 * C] = w
    for copy in copies:
        copy.wait()
    count = 2 * HELD_ROWS * 8
    for j in range(8):
        width = min(256, CELLS * C_IN - 128 * j)
        rows = raw[:, :, :, 128 * j : 128 * j + width].reshape(count, width)
        part = jnp.dot(
            rows, weights[j, 0:width, :].astype(jnp.bfloat16), preferred_element_type=jnp.float32
        )
        mixed[pl.ds(j, count, stride=8), :] = part
    starts = []
    for i in range(n_lat):
        top = r0 + PR * i - 1
        r_first = top + (a - top + 512) % n_lat
        lr = (r_first + 8) // 8 - 1 - low
        for m in range(MOST):
            starts.append(jnp.clip(lr + m, 0, HELD_ROWS - 1) * 8)

    def one_column(j, carry):
        left = c0 + PC * j - 1
        d = (b - left + 16 * CB_COLS) % n_lon
        n = (left + d - c_first) // n_lon
        pos = jnp.minimum(lc_first % 8 + n, 15)
        base = (pos // 8) * (HELD_ROWS * 8) + pos % 8
        for i in range(n_lat):
            for m in range(MOST):
                at = (base + starts[i * MOST + m]) * 8
                block = mixed[pl.ds(pl.multiple_of(at, 8), 8), :]
                out_ref[(i * n_lon + j) * MOST + m] = block.astype(jnp.bfloat16)
        return carry

    lax.fori_loop(0, n_lon, one_column, 0)


def pack(block_ids, coarse, w_mix):
    return pl.pallas_call(
        pack_body,
        out_shape=jax.ShapeDtypeStruct((128 * MOST, 8, 128), jnp.bfloat16),
        grid=(1,),
        in_specs=[
            pl.BlockSpec((8, 128), lambda g: (0, 0), memory_space=pltpu.SMEM),
            pl.BlockSpec(memory_space=pl.ANY),
            pl.BlockSpec((C, C_IN), lambda g: (0, 0)),
        ],
        out_specs=pl.BlockSpec((128 * MOST, 8, 128), lambda g: (0, 0, 0)),
        scratch_shapes=[
            pltpu.VMEM((2, HELD_ROWS, 8, CELLS * C_IN), jnp.bfloat16),
            pltpu.VMEM((8, 256, 2 * C), jnp.float32),
            pltpu.VMEM((2 * HELD_ROWS * 8 * 8, 128), jnp.float32),
            pltpu.SemaphoreType.DMA((2,)),
        ],
        name="pack",
    )(block_ids.T, coarse.reshape(CB_ROWS, CB_COLS, CELLS * C_IN), w_mix.T)


def fine_body(
    where_ref, bias_ref, land_ref, inc_hbm, spread_hbm, taps_hbm, out_hbm,
    inc, spread, taps, cells, cells_t, field, halo, bias, outs, in_sems, out_sems,
):
    loads = []
    for n, (source, target) in enumerate(((inc_hbm, inc), (spread_hbm, spread), (taps_hbm, taps))):
        load = pltpu.make_async_copy(source, target, in_sems.at[n])
        load.start()
        loads.append(load)
    for o in range(C):
        bias[o] = jnp.full((8, 128), bias_ref[o], jnp.float32)
    lower = lax.broadcasted_iota(jnp.int32, (8, 128), 1) < C
    loads[0].wait()
    for q in range(WR // 2):
        for col in range(WC):
            got = []
            for half in range(2):
                at = where_ref[(2 * q + half) * WC + col]
                block = inc[jnp.maximum(at, 0)].astype(jnp.float32)
                got.append(jnp.where(at >= 0, block, 0.0))
            u, v = got
            cells[q, 8 * col : 8 * col + 8, :] = jnp.where(lower, u, pltpu.roll(v, C, 1))
            cells[q, 8 * (WC + col) : 8 * (WC + col) + 8, :] = jnp.where(lower, pltpu.roll(u, C, 1), v)
    for q in range(WR // 2):
        cells_t[128 * q : 128 * q + 128, :] = cells[q].T.astype(jnp.bfloat16)
    loads[1].wait()

    def upsample(n, carry):
        right = jnp.concatenate([spread[4 * n + q] for q in range(4)], axis=1)
        fine = jnp.dot(
            cells_t[:, 0 : CELLS * WC], right, preferred_element_type=jnp.float32
        ).astype(jnp.bfloat16)
        for q in range(4):
            field[:, 4 * n + q] = fine[:, 128 * q : 128 * q + 128].reshape(WR, C, 128)
        return carry

    lax.fori_loop(0, 4, upsample, 0)
    edge = jnp.dot(cells_t[:, 0 : CELLS * WC], spread[16], preferred_element_type=jnp.float32)
    halo[...] = edge.astype(jnp.bfloat16).reshape(WR, C, 128)
    loads[2].wait()
    lane = lax.broadcasted_iota(jnp.int32, (C, 128), 1)
    spot = lax.broadcasted_iota(jnp.int32, (16, 8, 128), 1) // 2

    def band(step):
        centre = []
        left = []
        right = []
        for rr in range(18):
            row = 15 + rr
            mid = field[step + row // 16, row % 16]
            side = pltpu.roll(halo[step + row // 16], 127 - 2 * (row % 16), 1)
            centre.append(mid)
            left.append(jnp.where(lane == 0, side, pltpu.roll(mid, 1, 1)))
            right.append(jnp.where(lane == 127, side, pltpu.roll(mid, 127, 1)))
        totals = []
        for k in range(4):
            columns = []
            for hb in range(2):
                at = 2 * (4 * hb + k)
                columns.append(
                    jnp.concatenate(left[at : at + 4] + centre[at : at + 4] + right[at : at + 4], axis=0)
                )
            totals.append(
                jnp.dot(taps[k], jnp.concatenate(columns, axis=1), preferred_element_type=jnp.float32)
            )
        land = land_ref[pl.ds(step, 1), :]
        for u in range(4):
            halves = []
            for hb in range(2):
                t = [total[:, 128 * hb : 128 * hb + 128].reshape(16, 8, 128) for total in totals]
                got = t[3]
                for k in range(3):
                    got = jnp.where(spot == (u + k) % 4, t[k], got)
                if u > 0:
                    got = pltpu.roll(got, 8 - 2 * u, 1)
                halves.append((got + bias[16 * u : 16 * u + 16]) * land)
            outs[step, :, u] = jnp.concatenate(halves, axis=1).astype(jnp.bfloat16)

    def store(step):
        rows = pl.ds(step * 16 if isinstance(step, int) else pl.multiple_of(step * 16, 16), 16)
        return pltpu.make_async_copy(outs.at[step], out_hbm.at[:, :, rows, :], out_sems.at[step])

    def two_bands(t, carry):
        for half in range(2):
            step = 2 * t + half
            band(step)
            store(step).start()
        return carry

    lax.fori_loop(0, PR // 2, two_bands, 0)
    for step in range(PR):
        store(step).wait()


def fine(where, bias_order, land, incoming, spread, taps):
    return pl.pallas_call(
        fine_body,
        out_shape=jax.ShapeDtypeStruct((C // 4, 4, PR * 16, 128), jnp.bfloat16),
        in_specs=[
            pl.BlockSpec(memory_space=pltpu.SMEM),
            pl.BlockSpec(memory_space=pltpu.SMEM),
            pl.BlockSpec(memory_space=pltpu.VMEM),
            pl.BlockSpec(memory_space=pl.ANY),
            pl.BlockSpec(memory_space=pl.ANY),
            pl.BlockSpec(memory_space=pl.ANY),
        ],
        out_specs=pl.BlockSpec(memory_space=pl.ANY),
        scratch_shapes=[
            pltpu.VMEM((128 * MOST, 8, 128), jnp.bfloat16),
            pltpu.VMEM((17, CELLS * WC, 128), jnp.bfloat16),
            pltpu.VMEM((4, 2 * C, 12 * C), jnp.bfloat16),
            pltpu.VMEM((WR // 2, 256, 128), jnp.float32),
            pltpu.VMEM((WR * C, 256), jnp.bfloat16),
            pltpu.VMEM((WR, 16, C, 128), jnp.bfloat16),
            pltpu.VMEM((WR, C, 128), jnp.bfloat16),
            pltpu.VMEM((C, 8, 128), jnp.float32),
            pltpu.VMEM((PR, C // 4, 4, 16, 128), jnp.bfloat16),
            pltpu.SemaphoreType.DMA((3,)),
            pltpu.SemaphoreType.DMA((PR,)),
        ],
        name="fine",
    )(where, bias_order, land, incoming, spread, taps)


def spread_of(interp):
    cells = interp.reshape(8, 2, 16, 16).transpose(2, 1, 0, 3)
    wide = jnp.tile(cells, (1, 1, 1, PC))
    same = jnp.arange(128)[None, :] // 16 + 1 == jnp.arange(WC)[:, None]
    inner = jnp.where(same[None, None, :, None, :], wide[:, :, None], 0)
    edges = jnp.stack([cells[..., 0], cells[..., 15]], axis=1).reshape(32, 2, 8).transpose(1, 2, 0)
    edges = jnp.pad(edges, ((0, 0), (0, 0), (0, 96)))
    column = jnp.where(jnp.arange(128) % 2 == 0, WC - 1, 0)
    same = column[None, :] == jnp.arange(WC)[:, None]
    outer = jnp.where(same[None, :, None, :], edges[:, None], 0)
    full = jnp.concatenate([inner, outer[None]], axis=0)
    return full.reshape(17, CELLS * WC, 128).astype(jnp.bfloat16)


def taps_of(kernel):
    by = kernel.transpose(2, 1, 0, 3)
    rows = jnp.stack([jnp.pad(by, ((0, 0), (0, 0), (r, 1 - r), (0, 0))) for r in range(2)], axis=1)
    rows = rows.reshape(C // 4, 4, 2, 12 * C)
    return jnp.stack([jnp.roll(rows, k, axis=1) for k in range(4)]).reshape(4, 2 * C, 12 * C)


def per_device(coarse, w_mix, interp, kernel, bias, block_ids, valid):
    n_lat, n_lon = 8, 16
    i = lax.axis_index("lat")
    j = lax.axis_index("lon")
    outgoing = pack(block_ids, coarse, w_mix)
    incoming = lax.all_to_all(outgoing, ("lat", "lon"), split_axis=0, concat_axis=0, tiled=True)
    first = block_ids[0, 0]
    owner = first // (CB_ROWS * CB_COLS)
    local = first % (CB_ROWS * CB_COLS)
    r0 = (local // CB_COLS) * n_lat + owner // n_lon
    c0 = (local % CB_COLS) * n_lon + owner % n_lon
    grid = valid.reshape(n_lat, n_lon, PR, PC).transpose(0, 2, 1, 3).reshape(n_lat * PR, n_lon * PC)
    window = lax.dynamic_slice(jnp.pad(grid, 1), (i * PR, j * PC), (WR, WC))
    row = jnp.arange(WR)[:, None]
    col = jnp.arange(WC)[None, :]
    source = (r0 + PR * i - 1 + row + 8) % n_lat * n_lon + (c0 + PC * j - 1 + col + 16) % n_lon
    where = jnp.where(window > 0, source * MOST + row // 8, -1).reshape(WR * WC).astype(jnp.int32)
    own = window[1:-1, 1:-1].astype(jnp.float32)
    land = jnp.repeat(own, 16, axis=1)
    bias_order = bias.reshape(C // 4, 4).T.reshape(C)
    out = fine(where, bias_order, land, incoming, spread_of(interp), taps_of(kernel))
    return out.reshape(C, PR * 16, 128)


def solution(mesh):
    placed = (P(("lat", "lon"), None), P(), P(), P(), P(), P(), P())
    return jax.shard_map(
        per_device, mesh=mesh, in_specs=placed, out_specs=P(None, "lat", "lon"), check_vma=False
    )
```

```python
import jax
import jax.numpy as jnp
from jax import lax
from jax.experimental import pallas as pl
from jax.experimental.pallas import tpu as pltpu
from jax.sharding import PartitionSpec as P

PR = 18
PC = 8
CELLS = 16
WR = PR + 2
WC = PC + 2
MOST = 3
CB_ROWS = 24
CB_COLS = 40
HELD_ROWS = 20
C_IN = 69
C = 64
GRID_COLS = 640


def pack_body(ids_ref, coarse_ref, w_ref, out_ref, raw, weights, mixed, sems):
    n_lat, n_lon = 8, 16
    a = lax.axis_index("lat")
    b = lax.axis_index("lon")
    first = ids_ref[0, 0]
    owner = first // (CB_ROWS * CB_COLS)
    local = first % (CB_ROWS * CB_COLS)
    r0 = (local // CB_COLS) * n_lat + owner // n_lon
    c0 = (local % CB_COLS) * n_lon + owner % n_lon
    low = jnp.clip((r0 + 7) // 8 - 1, 0, CB_ROWS - HELD_ROWS)
    c_first = c0 - 1 + (b - c0 + 1 + 16 * CB_COLS) % n_lon
    lc_first = ((c_first + GRID_COLS) % GRID_COLS) // n_lon
    tile0 = lc_first // 8
    tile1 = (tile0 + 1) % (CB_COLS // 8)
    copies = []
    for slot, tile in ((0, tile0), (1, tile1)):
        copy = pltpu.make_async_copy(
            coarse_ref.at[pl.ds(low, HELD_ROWS), pl.ds(pl.multiple_of(tile * 8, 8), 8), :],
            raw.at[slot],
            sems.at[slot],
        )
        copy.start()
        copies.append(copy)
    w = w_ref[...].astype(jnp.float32).T
    weights[...] = jnp.zeros_like(weights)
    for j in range(8):
        weights[j, 10 * j : 10 * j + C_IN, 0:C] = w
        weights[j, 10 * j + C_IN : 10 * j + 2 * C_IN, C : 2 * C] = w
    for copy in copies:
        copy.wait()
    count = 2 * HELD_ROWS * 8
    for j in range(8):
        width = min(256, CELLS * C_IN - 128 * j)
        rows = raw[:, :, :, 128 * j : 128 * j + width].reshape(count, width)
        part = jnp.dot(
            rows, weights[j, 0:width, :].astype(jnp.bfloat16), preferred_element_type=jnp.float32
        )
        mixed[pl.ds(j, count, stride=8), :] = part
    starts = []
    for i in range(n_lat):
        top = r0 + PR * i - 1
        r_first = top + (a - top + 512) % n_lat
        lr = (r_first + 8) // 8 - 1 - low
        for m in range(MOST):
            starts.append(jnp.clip(lr + m, 0, HELD_ROWS - 1) * 64)
    for j in range(n_lon):
        left = c0 + PC * j - 1
        d = (b - left + 16 * CB_COLS) % n_lon
        n = (left + d - c_first) // n_lon
        pos = jnp.minimum(lc_first % 8 + n, 15)
        base = ((pos // 8) * (HELD_ROWS * 8) + pos % 8) * 8
        for i in range(n_lat):
            for m in range(MOST):
                block = mixed[pl.ds(pl.multiple_of(base + starts[i * MOST + m], 8), 8), :]
                out_ref[(i * n_lon + j) * MOST + m] = block.astype(jnp.bfloat16)


def pack(block_ids, coarse, w_mix):
    return pl.pallas_call(
        pack_body,
        out_shape=pltpu.VMEM((128 * MOST, 8, 128), jnp.bfloat16),
        grid=(1,),
        in_specs=[
            pl.BlockSpec((8, 128), lambda g: (0, 0), memory_space=pltpu.SMEM),
            pl.BlockSpec(memory_space=pl.ANY),
            pl.BlockSpec((C, C_IN), lambda g: (0, 0)),
        ],
        out_specs=pl.BlockSpec(memory_space=pltpu.VMEM),
        scratch_shapes=[
            pltpu.VMEM((2, HELD_ROWS, 8, CELLS * C_IN), jnp.bfloat16),
            pltpu.VMEM((8, 256, 2 * C), jnp.float32),
            pltpu.VMEM((2 * HELD_ROWS * 8 * 8, 128), jnp.float32),
            pltpu.SemaphoreType.DMA((2,)),
        ],
        compiler_params=pltpu.CompilerParams(vmem_limit_bytes=40 << 20),
        name="pack",
    )(block_ids, coarse, w_mix)


def fine_body(
    where_ref, bias_ref, land_ref, inc, spread, taps, out_hbm,
    cells, cells_t, field, halo, bias, outs, out_sems,
):
    for o in range(C):
        bias[o] = jnp.full((8, 128), bias_ref[o], jnp.float32)
    lower = lax.broadcasted_iota(jnp.int32, (8, 128), 1) < C
    for q in range(WR // 2):
        for col in range(WC):
            got = []
            for half in range(2):
                at = where_ref[(2 * q + half) * WC + col]
                block = inc[jnp.maximum(at, 0)].astype(jnp.float32)
                got.append(jnp.where(at >= 0, block, 0.0))
            u, v = got
            cells[q, 8 * col : 8 * col + 8, :] = jnp.where(lower, u, pltpu.roll(v, C, 1))
            cells[q, 8 * (WC + col) : 8 * (WC + col) + 8, :] = jnp.where(lower, pltpu.roll(u, C, 1), v)
    for q in range(WR // 2):
        cells_t[128 * q : 128 * q + 128, :] = cells[q].T.astype(jnp.bfloat16)

    edge = jnp.dot(cells_t[:, 0 : CELLS * WC], spread[16], preferred_element_type=jnp.float32)
    halo[...] = edge.astype(jnp.bfloat16)
    lane = lax.broadcasted_iota(jnp.int32, (WR * C, 128), 1)
    for n in range(4):
        wide = jnp.concatenate([spread[4 * n + q] for q in range(4)], axis=1)
        fine = jnp.dot(
            cells_t[:, 0 : CELLS * WC], wide, preferred_element_type=jnp.float32
        ).astype(jnp.bfloat16)
        for q in range(4):
            row = 4 * n + q
            mid = fine[:, 128 * q : 128 * q + 128]
            side = pltpu.roll(halo[...], 127 - 2 * row, 1)
            left = jnp.where(lane == 0, side, pltpu.roll(mid, 1, 1))
            right = jnp.where(lane == 127, side, pltpu.roll(mid, 127, 1))
            for tap, part in enumerate((left, mid, right)):
                field[tap, :, row] = part.reshape(WR, C, 128)
    spot = lax.broadcasted_iota(jnp.int32, (16, 8, 128), 1) // 2

    def band(step):
        totals = []
        for k in range(4):
            columns = []
            for hb in range(2):
                at = 2 * (4 * hb + k)
                parts = []
                for tap in range(3):
                    for rr in range(at, at + 4):
                        row = 15 + rr
                        parts.append(field[tap, step + row // 16, row % 16])
                columns.append(jnp.concatenate(parts, axis=0))
            totals.append(
                jnp.dot(taps[k], jnp.concatenate(columns, axis=1), preferred_element_type=jnp.float32)
            )
        land = land_ref[step : step + 1, :]
        for u in range(4):
            halves = []
            for hb in range(2):
                t = [total[:, 128 * hb : 128 * hb + 128].reshape(16, 8, 128) for total in totals]
                got = t[3]
                for k in range(3):
                    got = jnp.where(spot == (u + k) % 4, t[k], got)
                if u > 0:
                    got = pltpu.roll(got, 8 - 2 * u, 1)
                halves.append((got + bias[16 * u : 16 * u + 16]) * land)
            outs[step, :, u] = jnp.concatenate(halves, axis=1).astype(jnp.bfloat16)

    def store(step):
        return pltpu.make_async_copy(
            outs.at[step], out_hbm.at[:, :, step * 16 : step * 16 + 16, :], out_sems.at[step]
        )

    for step in range(PR):
        band(step)
        store(step).start()
    for step in range(PR):
        store(step).wait()


def fine(where, bias_order, land, incoming, spread, taps):
    return pl.pallas_call(
        fine_body,
        out_shape=jax.ShapeDtypeStruct((C // 4, 4, PR * 16, 128), jnp.bfloat16),
        in_specs=[
            pl.BlockSpec(memory_space=pltpu.SMEM),
            pl.BlockSpec(memory_space=pltpu.SMEM),
            pl.BlockSpec(memory_space=pltpu.VMEM),
            pl.BlockSpec(memory_space=pltpu.VMEM),
            pl.BlockSpec(memory_space=pltpu.VMEM),
            pl.BlockSpec(memory_space=pltpu.VMEM),
        ],
        out_specs=pl.BlockSpec(memory_space=pl.ANY),
        scratch_shapes=[
            pltpu.VMEM((WR // 2, 256, 128), jnp.float32),
            pltpu.VMEM((WR * C, 256), jnp.bfloat16),
            pltpu.VMEM((3, WR, 16, C, 128), jnp.bfloat16),
            pltpu.VMEM((WR * C, 128), jnp.bfloat16),
            pltpu.VMEM((C, 8, 128), jnp.float32),
            pltpu.VMEM((PR, C // 4, 4, 16, 128), jnp.bfloat16),
            pltpu.SemaphoreType.DMA((PR,)),
        ],
        compiler_params=pltpu.CompilerParams(vmem_limit_bytes=40 << 20),
        name="fine",
    )(where, bias_order, land, incoming, spread, taps)


def spread_of(interp):
    cells = interp.reshape(8, 2, 16, 16).transpose(2, 1, 0, 3)
    wide = jnp.tile(cells, (1, 1, 1, PC))
    same = jnp.arange(128)[None, :] // 16 + 1 == jnp.arange(WC)[:, None]
    inner = jnp.where(same[None, None, :, None, :], wide[:, :, None], 0)
    edges = jnp.stack([cells[..., 0], cells[..., 15]], axis=1).reshape(32, 2, 8).transpose(1, 2, 0)
    edges = jnp.pad(edges, ((0, 0), (0, 0), (0, 96)))
    column = jnp.where(jnp.arange(128) % 2 == 0, WC - 1, 0)
    same = column[None, :] == jnp.arange(WC)[:, None]
    outer = jnp.where(same[None, :, None, :], edges[:, None], 0)
    full = jnp.concatenate([inner, outer[None]], axis=0)
    return full.reshape(17, CELLS * WC, 128).astype(jnp.bfloat16)


def taps_of(kernel):
    by = kernel.transpose(2, 1, 0, 3)
    rows = jnp.stack([jnp.pad(by, ((0, 0), (0, 0), (r, 1 - r), (0, 0))) for r in range(2)], axis=1)
    rows = rows.reshape(C // 4, 4, 2, 12 * C)
    return jnp.stack([jnp.roll(rows, k, axis=1) for k in range(4)]).reshape(4, 2 * C, 12 * C)


def per_device(coarse, w_mix, interp, kernel, bias, block_ids, valid):
    n_lat, n_lon = 8, 16
    i = lax.axis_index("lat")
    j = lax.axis_index("lon")
    far = (pltpu.with_memory_space_constraint(v, pltpu.HBM) for v in (block_ids.T, coarse.reshape(CB_ROWS, CB_COLS, CELLS * C_IN), w_mix.T))
    outgoing = pack(*far)
    incoming = lax.all_to_all(outgoing, ("lat", "lon"), split_axis=0, concat_axis=0, tiled=True)
    first = block_ids[0, 0]
    owner = first // (CB_ROWS * CB_COLS)
    local = first % (CB_ROWS * CB_COLS)
    r0 = (local // CB_COLS) * n_lat + owner // n_lon
    c0 = (local % CB_COLS) * n_lon + owner % n_lon
    grid = valid.reshape(n_lat, n_lon, PR, PC).transpose(0, 2, 1, 3).reshape(n_lat * PR, n_lon * PC)
    window = lax.dynamic_slice(jnp.pad(grid, 1), (i * PR, j * PC), (WR, WC))
    row = jnp.arange(WR)[:, None]
    col = jnp.arange(WC)[None, :]
    source = (r0 + PR * i - 1 + row + 8) % n_lat * n_lon + (c0 + PC * j - 1 + col + 16) % n_lon
    where = jnp.where(window > 0, source * MOST + row // 8, -1).reshape(WR * WC).astype(jnp.int32)
    own = window[1:-1, 1:-1].astype(jnp.float32)
    land = jnp.repeat(own, 16, axis=1)
    bias_order = bias.reshape(C // 4, 4).T.reshape(C)
    near = (land, incoming, spread_of(interp), taps_of(kernel))
    near = tuple(pltpu.with_memory_space_constraint(v, pltpu.VMEM) for v in near)
    out = fine(where, bias_order, *near)
    return out.reshape(C, PR * 16, 128)


def solution(mesh):
    placed = (P(("lat", "lon"), None), P(), P(), P(), P(), P(), P())
    return jax.shard_map(
        per_device, mesh=mesh, in_specs=placed, out_specs=P(None, "lat", "lon"), check_vma=False
    )
```

```python
import jax
import jax.numpy as jnp
from jax import lax
from jax.experimental import pallas as pl
from jax.experimental.pallas import tpu as pltpu
from jax.sharding import PartitionSpec as P

PR = 18
PC = 8
CELLS = 16
WR = PR + 2
WC = PC + 2
MOST = 3
CB_ROWS = 24
CB_COLS = 40
HELD_ROWS = 20
PART_ROWS = 10
C_IN = 69
CHUNK = 4
STEP = 4
C = 64
GRID_COLS = 640


def pack_body(
    ids_hbm, coarse_hbm, w_hbm, out_hbm, ids_ref, w_ref, raw, weights, mixed, outgoing, in_sems, out_sems
):
    n_lat, n_lon = 8, 16
    ids_copy = pltpu.make_async_copy(ids_hbm.at[0:8, :], ids_ref, in_sems.at[4])
    ids_copy.start()
    copies = []
    for part in range(4):
        rows = slice(6 * part, 6 * part + 6)
        copy = pltpu.make_async_copy(coarse_hbm.at[rows], raw.at[rows], in_sems.at[part])
        copy.start()
        copies.append(copy)
    w_copy = pltpu.make_async_copy(w_hbm, w_ref, in_sems.at[5])
    w_copy.start()
    ids_copy.wait()
    a = lax.axis_index("lat")
    b = lax.axis_index("lon")
    first = ids_ref[0, 0]
    owner = first // (CB_ROWS * CB_COLS)
    local = first % (CB_ROWS * CB_COLS)
    r0 = (local // CB_COLS) * n_lat + owner // n_lon
    c0 = (local % CB_COLS) * n_lon + owner % n_lon
    low = jnp.clip((r0 + 7) // 8 - 1, 0, CB_ROWS - HELD_ROWS)
    c_first = c0 - 1 + (b - c0 + 1 + 16 * CB_COLS) % n_lon
    lc_first = ((c_first + GRID_COLS) % GRID_COLS) // n_lon
    tile0 = lc_first // 8
    tile1 = (tile0 + 1) % (CB_COLS // 8)
    w_copy.wait()
    w = w_ref[...].astype(jnp.float32).T
    weights[...] = jnp.zeros_like(weights)
    for j in range(8):
        weights[j, 10 * j : 10 * j + C_IN, 0:C] = w
        weights[j, 10 * j + C_IN : 10 * j + 2 * C_IN, C : 2 * C] = w
    bases = []
    for j in range(n_lon):
        left = c0 + PC * j - 1
        d = (b - left + 16 * CB_COLS) % n_lon
        n = (left + d - c_first) // n_lon
        pos = jnp.minimum(lc_first % 8 + n, 15)
        bases.append(((pos // 8) * (PART_ROWS * 8) + pos % 8) * 8)
    count = 2 * PART_ROWS * 8

    def mix(part):
        for copy in copies[3 * part : 3 * part + 3]:
            copy.wait()
        top = low + PART_ROWS * part
        for j in range(8):
            width = min(256, CELLS * C_IN - 128 * j)
            rows = jnp.concatenate(
                [
                    raw[
                        pl.ds(top, PART_ROWS), pl.ds(pl.multiple_of(tile * 8, 8), 8), 128 * j : 128 * j + width
                    ].reshape(PART_ROWS * 8, width)
                    for tile in (tile0, tile1)
                ],
                axis=0,
            )
            mixed[pl.ds(part * count * 8 + j, count, stride=8), :] = jnp.dot(
                rows, weights[j, 0:width, :].astype(jnp.bfloat16), preferred_element_type=jnp.float32
            )

    def send(i):
        top = r0 + PR * i - 1
        r_first = top + (a - top + 512) % n_lat
        lr = (r_first + 8) // 8 - 1 - low
        for m in range(MOST):
            row = jnp.clip(lr + m, 0, HELD_ROWS - 1)
            start = (row + (row // PART_ROWS) * PART_ROWS) * 64
            for j in range(n_lon):
                block = mixed[pl.ds(pl.multiple_of(bases[j] + start, 8), 8), :]
                outgoing[(i * n_lon + j) * MOST + m] = block.astype(jnp.bfloat16)
        rows = slice(i * n_lon * MOST, (i + 1) * n_lon * MOST)
        copy = pltpu.make_async_copy(outgoing.at[rows], out_hbm.at[rows], out_sems.at[i])
        copy.start()
        return copy

    mix(0)
    sent = [send(i) for i in range(3)]
    mix(1)
    sent += [send(i) for i in range(3, n_lat)]
    for copy in sent:
        copy.wait()


def pack(block_ids, coarse, w_mix):
    return pl.pallas_call(
        pack_body,
        out_shape=jax.ShapeDtypeStruct((128 * MOST, 8, 128), jnp.bfloat16),
        in_specs=[
            pl.BlockSpec(memory_space=pl.ANY),
            pl.BlockSpec(memory_space=pl.ANY),
            pl.BlockSpec(memory_space=pl.ANY),
        ],
        out_specs=pl.BlockSpec(memory_space=pl.ANY),
        scratch_shapes=[
            pltpu.SMEM((8, 128), jnp.int32),
            pltpu.VMEM((C, C_IN), jnp.bfloat16),
            pltpu.VMEM((CB_ROWS, CB_COLS, CELLS * C_IN), jnp.bfloat16),
            pltpu.VMEM((8, 256, 2 * C), jnp.float32),
            pltpu.VMEM((2 * HELD_ROWS * 8 * 8, 128), jnp.float32),
            pltpu.VMEM((128 * MOST, 8, 128), jnp.bfloat16),
            pltpu.SemaphoreType.DMA((6,)),
            pltpu.SemaphoreType.DMA((8,)),
        ],
        compiler_params=pltpu.CompilerParams(vmem_limit_bytes=40 << 20),
        name="pack",
    )(block_ids, coarse, w_mix)


def fine_body(
    where_ref, bias_ref, land_ref, inc, spread, taps, out_hbm,
    cells, cells_t, field, halo, bias, outs, out_sems,
):
    for o in range(C):
        bias[o] = jnp.full((8, 128), bias_ref[o], jnp.float32)
    lower = lax.broadcasted_iota(jnp.int32, (8, 128), 1) < C

    def gather(q):
        for col in range(WC):
            got = []
            for half in range(2):
                at = where_ref[(2 * q + half) * WC + col]
                block = inc[jnp.maximum(at, 0)].astype(jnp.float32)
                got.append(jnp.where(at >= 0, block, 0.0))
            u, v = got
            cells[q, 8 * col : 8 * col + 8, :] = jnp.where(lower, u, pltpu.roll(v, C, 1))
            cells[q, 8 * (WC + col) : 8 * (WC + col) + 8, :] = jnp.where(lower, pltpu.roll(u, C, 1), v)
        cells_t[128 * q : 128 * q + 128, :] = cells[q].T.astype(jnp.bfloat16)

    def edges(lo, hi):
        side = jnp.dot(
            cells_t[C * lo : C * hi, 0 : CELLS * WC], spread[16], preferred_element_type=jnp.float32
        )
        halo[C * lo : C * hi, :] = side.astype(jnp.bfloat16)

    def upsample(lo, hi, first, count):
        lane = lax.broadcasted_iota(jnp.int32, ((hi - lo) * C, 128), 1)
        wide = jnp.concatenate([spread[first + q] for q in range(count)], axis=1)
        fine = jnp.dot(
            cells_t[C * lo : C * hi, 0 : CELLS * WC], wide, preferred_element_type=jnp.float32
        ).astype(jnp.bfloat16)
        for q in range(count):
            row = first + q
            mid = fine[:, 128 * q : 128 * q + 128]
            side = pltpu.roll(halo[C * lo : C * hi, :], 127 - 2 * row, 1)
            left = jnp.where(lane == 0, side, pltpu.roll(mid, 1, 1))
            right = jnp.where(lane == 127, side, pltpu.roll(mid, 127, 1))
            for tap, part in enumerate((left, mid, right)):
                field[tap, lo:hi, row] = part.reshape(hi - lo, C, 128)

    def pieces(lo, hi):
        def first_piece():
            for q in range(lo // 2, hi // 2):
                gather(q)
            edges(lo, hi)

        yield first_piece
        for first in range(0, 16, STEP):
            low = max(lo, 1) if first + STEP <= 15 else lo
            high = min(hi, WR - 1) if first > 0 else hi
            yield lambda low=low, high=high, first=first: upsample(low, high, first, STEP)

    spot = lax.broadcasted_iota(jnp.int32, (8, 128), 0) // 2

    def band(step):
        totals = []
        for k in range(4):
            columns = []
            for hb in range(2):
                at = 2 * (4 * hb + k)
                parts = []
                for tap in range(3):
                    for rr in range(at, at + 4):
                        row = 15 + rr
                        parts.append(field[tap, step + row // 16, row % 16])
                columns.append(jnp.concatenate(parts, axis=0))
            totals.append(
                jnp.dot(taps[k], jnp.concatenate(columns, axis=1), preferred_element_type=jnp.float32)
            )
        land = land_ref[step : step + 1, :]
        for v in range(C // 4):
            for u in range(4):
                halves = []
                for hb in range(2):
                    t = [total[8 * v : 8 * v + 8, 128 * hb : 128 * hb + 128] for total in totals]
                    got = t[3]
                    for k in range(3):
                        got = jnp.where(spot == (u + k) % 4, t[k], got)
                    if u > 0:
                        got = pltpu.roll(got, 8 - 2 * u, 0)
                    halves.append((got + bias[16 * u + v]) * land)
                outs[4 * v + u, 16 * step : 16 * step + 16, :] = jnp.concatenate(halves, axis=0).astype(jnp.bfloat16)

    def store(step):
        rows = slice(step * 16, step * 16 + 16)
        return pltpu.make_async_copy(outs.at[:, rows, :], out_hbm.at[:, rows, :], out_sems.at[step])

    for piece in pieces(0, CHUNK):
        piece()
    done = 0
    for lo in range(CHUNK, WR + CHUNK, CHUNK):
        ready = min(lo - 2, PR)
        todo = list(pieces(lo, lo + CHUNK)) if lo < WR else []
        count = ready - done
        for n, step in enumerate(range(done, ready)):
            for piece in todo[n * len(todo) // count : (n + 1) * len(todo) // count]:
                piece()
            band(step)
            store(step).start()
        done = ready
    for step in range(PR):
        store(step).wait()


def fine(where, bias_order, land, incoming, spread, taps):
    return pl.pallas_call(
        fine_body,
        out_shape=jax.ShapeDtypeStruct((C, PR * 16, 128), jnp.bfloat16),
        in_specs=[
            pl.BlockSpec(memory_space=pltpu.SMEM),
            pl.BlockSpec(memory_space=pltpu.SMEM),
            pl.BlockSpec(memory_space=pltpu.VMEM),
            pl.BlockSpec(memory_space=pltpu.VMEM),
            pl.BlockSpec(memory_space=pltpu.VMEM),
            pl.BlockSpec(memory_space=pltpu.VMEM),
        ],
        out_specs=pl.BlockSpec(memory_space=pl.ANY),
        scratch_shapes=[
            pltpu.VMEM((WR // 2, 256, 128), jnp.float32),
            pltpu.VMEM((WR * C, 256), jnp.bfloat16),
            pltpu.VMEM((3, WR, 16, C, 128), jnp.bfloat16),
            pltpu.VMEM((WR * C, 128), jnp.bfloat16),
            pltpu.VMEM((C, 8, 128), jnp.float32),
            pltpu.VMEM((C, PR * 16, 128), jnp.bfloat16),
            pltpu.SemaphoreType.DMA((PR,)),
        ],
        compiler_params=pltpu.CompilerParams(vmem_limit_bytes=40 << 20),
        name="fine",
    )(where, bias_order, land, incoming, spread, taps)


def spread_of(interp):
    cells = interp.reshape(8, 2, 16, 16).transpose(2, 1, 0, 3)
    wide = jnp.tile(cells, (1, 1, 1, PC))
    same = jnp.arange(128)[None, :] // 16 + 1 == jnp.arange(WC)[:, None]
    inner = jnp.where(same[None, None, :, None, :], wide[:, :, None], 0)
    edges = jnp.stack([cells[..., 0], cells[..., 15]], axis=1).reshape(32, 2, 8).transpose(1, 2, 0)
    edges = jnp.pad(edges, ((0, 0), (0, 0), (0, 96)))
    column = jnp.where(jnp.arange(128) % 2 == 0, WC - 1, 0)
    same = column[None, :] == jnp.arange(WC)[:, None]
    outer = jnp.where(same[None, :, None, :], edges[:, None], 0)
    full = jnp.concatenate([inner, outer[None]], axis=0)
    return full.reshape(17, CELLS * WC, 128).astype(jnp.bfloat16)


def taps_of(kernel):
    by = kernel.transpose(2, 1, 0, 3)
    rows = jnp.stack([jnp.pad(by, ((0, 0), (0, 0), (r, 1 - r), (0, 0))) for r in range(2)], axis=1)
    rows = rows.reshape(C // 4, 4, 2, 12 * C)
    return jnp.stack([jnp.roll(rows, k, axis=1) for k in range(4)]).reshape(4, 2 * C, 12 * C)


def per_device(coarse, w_mix, interp, kernel, bias, block_ids, valid):
    n_lat, n_lon = 8, 16
    i = lax.axis_index("lat")
    j = lax.axis_index("lon")
    far = (pltpu.with_memory_space_constraint(v, pltpu.HBM) for v in (block_ids.T, coarse.reshape(CB_ROWS, CB_COLS, CELLS * C_IN), w_mix.T))
    outgoing = pack(*far)
    incoming = lax.all_to_all(outgoing, ("lat", "lon"), split_axis=0, concat_axis=0, tiled=True)
    first = block_ids[0, 0]
    owner = first // (CB_ROWS * CB_COLS)
    local = first % (CB_ROWS * CB_COLS)
    r0 = (local // CB_COLS) * n_lat + owner // n_lon
    c0 = (local % CB_COLS) * n_lon + owner % n_lon
    grid = valid.reshape(n_lat, n_lon, PR, PC).transpose(0, 2, 1, 3).reshape(n_lat * PR, n_lon * PC)
    window = lax.dynamic_slice(jnp.pad(grid, 1), (i * PR, j * PC), (WR, WC))
    row = jnp.arange(WR)[:, None]
    col = jnp.arange(WC)[None, :]
    source = (r0 + PR * i - 1 + row + 8) % n_lat * n_lon + (c0 + PC * j - 1 + col + 16) % n_lon
    where = jnp.where(window > 0, source * MOST + row // 8, -1).reshape(WR * WC).astype(jnp.int32)
    own = window[1:-1, 1:-1].astype(jnp.float32)
    land = jnp.repeat(own, 16, axis=1)
    bias_order = bias.reshape(C // 4, 4).T.reshape(C)
    near = (land, incoming, spread_of(interp), taps_of(kernel))
    near = tuple(pltpu.with_memory_space_constraint(v, pltpu.VMEM) for v in near)
    return fine(where, bias_order, *near)


def solution(mesh):
    placed = (P(("lat", "lon"), None), P(), P(), P(), P(), P(), P())
    return jax.shard_map(
        per_device, mesh=mesh, in_specs=placed, out_specs=P(None, "lat", "lon"), check_vma=False
    )
```

```python
import jax
import jax.numpy as jnp
from jax import lax
from jax.experimental import pallas as pl
from jax.experimental.pallas import tpu as pltpu
from jax.sharding import PartitionSpec as P

PR = 18
PC = 8
CELLS = 16
WR = PR + 2
WC = PC + 2
MOST = 3
CB_ROWS = 24
CB_COLS = 40
HELD_ROWS = 20
PART_ROWS = 20
C_IN = 69
CHUNK = 4
STEP = 4
C = 64
GRID_COLS = 640


def pack_body(
    ids_hbm, coarse_hbm, w_hbm, out_hbm, ids_ref, w_ref, raw, weights, mixed, outgoing, in_sems, out_sems
):
    n_lat, n_lon = 8, 16
    ids_copy = pltpu.make_async_copy(ids_hbm.at[0:8, :], ids_ref, in_sems.at[4])
    ids_copy.start()
    copies = []
    for part in range(4):
        rows = slice(6 * part, 6 * part + 6)
        copy = pltpu.make_async_copy(coarse_hbm.at[rows], raw.at[rows], in_sems.at[part])
        copy.start()
        copies.append(copy)
    w_copy = pltpu.make_async_copy(w_hbm, w_ref, in_sems.at[5])
    w_copy.start()
    ids_copy.wait()
    a = lax.axis_index("lat")
    b = lax.axis_index("lon")
    first = ids_ref[0, 0]
    owner = first // (CB_ROWS * CB_COLS)
    local = first % (CB_ROWS * CB_COLS)
    r0 = (local // CB_COLS) * n_lat + owner // n_lon
    c0 = (local % CB_COLS) * n_lon + owner % n_lon
    low = jnp.clip((r0 + 7) // 8 - 1, 0, CB_ROWS - HELD_ROWS)
    c_first = c0 - 1 + (b - c0 + 1 + 16 * CB_COLS) % n_lon
    lc_first = ((c_first + GRID_COLS) % GRID_COLS) // n_lon
    tile0 = lc_first // 8
    tile1 = (tile0 + 1) % (CB_COLS // 8)
    w_copy.wait()
    w = w_ref[...].astype(jnp.float32).T
    weights[...] = jnp.zeros_like(weights)
    for j in range(8):
        weights[j, 10 * j : 10 * j + C_IN, 0:C] = w
        weights[j, 10 * j + C_IN : 10 * j + 2 * C_IN, C : 2 * C] = w
    bases = []
    for j in range(n_lon):
        left = c0 + PC * j - 1
        d = (b - left + 16 * CB_COLS) % n_lon
        n = (left + d - c_first) // n_lon
        pos = jnp.minimum(lc_first % 8 + n, 15)
        bases.append(((pos // 8) * (PART_ROWS * 8) + pos % 8) * 8)
    count = 2 * PART_ROWS * 8

    def mix(part):
        for copy in copies:
            copy.wait()
        top = low + PART_ROWS * part
        for j in range(8):
            width = min(256, CELLS * C_IN - 128 * j)
            rows = jnp.concatenate(
                [
                    raw[
                        pl.ds(top, PART_ROWS), pl.ds(pl.multiple_of(tile * 8, 8), 8), 128 * j : 128 * j + width
                    ].reshape(PART_ROWS * 8, width)
                    for tile in (tile0, tile1)
                ],
                axis=0,
            )
            mixed[pl.ds(part * count * 8 + j, count, stride=8), :] = jnp.dot(
                rows, weights[j, 0:width, :].astype(jnp.bfloat16), preferred_element_type=jnp.float32
            )

    def send(i):
        top = r0 + PR * i - 1
        r_first = top + (a - top + 512) % n_lat
        lr = (r_first + 8) // 8 - 1 - low
        for m in range(MOST):
            row = jnp.clip(lr + m, 0, HELD_ROWS - 1)
            start = (row + (row // PART_ROWS) * PART_ROWS) * 64
            for j in range(n_lon):
                block = mixed[pl.ds(pl.multiple_of(bases[j] + start, 8), 8), :]
                outgoing[(i * n_lon + j) * MOST + m] = block.astype(jnp.bfloat16)
        rows = slice(i * n_lon * MOST, (i + 1) * n_lon * MOST)
        copy = pltpu.make_async_copy(outgoing.at[rows], out_hbm.at[rows], out_sems.at[i])
        copy.start()
        return copy

    mix(0)
    sent = [send(i) for i in range(3)]
    sent += [send(i) for i in range(3, n_lat)]
    for copy in sent:
        copy.wait()


def pack(block_ids, coarse, w_mix):
    return pl.pallas_call(
        pack_body,
        out_shape=jax.ShapeDtypeStruct((128 * MOST, 8, 128), jnp.bfloat16),
        in_specs=[
            pl.BlockSpec(memory_space=pl.ANY),
            pl.BlockSpec(memory_space=pl.ANY),
            pl.BlockSpec(memory_space=pl.ANY),
        ],
        out_specs=pl.BlockSpec(memory_space=pl.ANY),
        scratch_shapes=[
            pltpu.SMEM((8, 128), jnp.int32),
            pltpu.VMEM((C, C_IN), jnp.bfloat16),
            pltpu.VMEM((CB_ROWS, CB_COLS, CELLS * C_IN), jnp.bfloat16),
            pltpu.VMEM((8, 256, 2 * C), jnp.float32),
            pltpu.VMEM((2 * HELD_ROWS * 8 * 8, 128), jnp.float32),
            pltpu.VMEM((128 * MOST, 8, 128), jnp.bfloat16),
            pltpu.SemaphoreType.DMA((6,)),
            pltpu.SemaphoreType.DMA((8,)),
        ],
        compiler_params=pltpu.CompilerParams(vmem_limit_bytes=40 << 20),
        name="pack",
    )(block_ids, coarse, w_mix)


def fine_body(
    where_ref, bias_ref, land_ref, inc, spread, taps, out_hbm,
    cells, cells_t, field, halo, bias, outs, out_sems,
):
    for o in range(C):
        bias[o] = jnp.full((8, 128), bias_ref[o], jnp.float32)
    lower = lax.broadcasted_iota(jnp.int32, (8, 128), 1) < C

    def gather(q):
        for col in range(WC):
            got = []
            for half in range(2):
                at = where_ref[(2 * q + half) * WC + col]
                block = inc[jnp.maximum(at, 0)].astype(jnp.float32)
                got.append(jnp.where(at >= 0, block, 0.0))
            u, v = got
            cells[q, 8 * col : 8 * col + 8, :] = jnp.where(lower, u, pltpu.roll(v, C, 1))
            cells[q, 8 * (WC + col) : 8 * (WC + col) + 8, :] = jnp.where(lower, pltpu.roll(u, C, 1), v)
        cells_t[128 * q : 128 * q + 128, :] = cells[q].T.astype(jnp.bfloat16)

    def edges(lo, hi):
        side = jnp.dot(
            cells_t[C * lo : C * hi, 0 : CELLS * WC], spread[16], preferred_element_type=jnp.float32
        )
        halo[C * lo : C * hi, :] = side.astype(jnp.bfloat16)

    def upsample(lo, hi, first, count):
        lane = lax.broadcasted_iota(jnp.int32, ((hi - lo) * C, 128), 1)
        wide = jnp.concatenate([spread[first + q] for q in range(count)], axis=1)
        fine = jnp.dot(
            cells_t[C * lo : C * hi, 0 : CELLS * WC], wide, preferred_element_type=jnp.float32
        ).astype(jnp.bfloat16)
        for q in range(count):
            row = first + q
            mid = fine[:, 128 * q : 128 * q + 128]
            side = pltpu.roll(halo[C * lo : C * hi, :], 127 - 2 * row, 1)
            left = jnp.where(lane == 0, side, pltpu.roll(mid, 1, 1))
            right = jnp.where(lane == 127, side, pltpu.roll(mid, 127, 1))
            for tap, part in enumerate((left, mid, right)):
                field[tap, lo:hi, row] = part.reshape(hi - lo, C, 128)

    def pieces(lo, hi):
        def first_piece():
            for q in range(lo // 2, hi // 2):
                gather(q)
            edges(lo, hi)

        yield first_piece
        for first in range(0, 16, STEP):
            low = max(lo, 1) if first + STEP <= 15 else lo
            high = min(hi, WR - 1) if first > 0 else hi
            yield lambda low=low, high=high, first=first: upsample(low, high, first, STEP)

    spot = lax.broadcasted_iota(jnp.int32, (8, 128), 0) // 2

    def band(step):
        totals = []
        for k in range(4):
            columns = []
            for hb in range(2):
                at = 2 * (4 * hb + k)
                parts = []
                for tap in range(3):
                    for rr in range(at, at + 4):
                        row = 15 + rr
                        parts.append(field[tap, step + row // 16, row % 16])
                columns.append(jnp.concatenate(parts, axis=0))
            totals.append(
                jnp.dot(taps[k], jnp.concatenate(columns, axis=1), preferred_element_type=jnp.float32)
            )
        land = land_ref[step : step + 1, :]
        for v in range(C // 4):
            for u in range(4):
                halves = []
                for hb in range(2):
                    t = [total[8 * v : 8 * v + 8, 128 * hb : 128 * hb + 128] for total in totals]
                    got = t[3]
                    for k in range(3):
                        got = jnp.where(spot == (u + k) % 4, t[k], got)
                    if u > 0:
                        got = pltpu.roll(got, 8 - 2 * u, 0)
                    halves.append((got + bias[16 * u + v]) * land)
                outs[4 * v + u, 16 * step : 16 * step + 16, :] = jnp.concatenate(halves, axis=0).astype(jnp.bfloat16)

    def store(step):
        rows = slice(step * 16, step * 16 + 16)
        return pltpu.make_async_copy(outs.at[:, rows, :], out_hbm.at[:, rows, :], out_sems.at[step])

    for piece in pieces(0, CHUNK):
        piece()
    done = 0
    for lo in range(CHUNK, WR + CHUNK, CHUNK):
        ready = min(lo - 2, PR)
        todo = list(pieces(lo, lo + CHUNK)) if lo < WR else []
        count = ready - done
        for n, step in enumerate(range(done, ready)):
            for piece in todo[n * len(todo) // count : (n + 1) * len(todo) // count]:
                piece()
            band(step)
            store(step).start()
        done = ready
    for step in range(PR):
        store(step).wait()


def fine(where, bias_order, land, incoming, spread, taps):
    return pl.pallas_call(
        fine_body,
        out_shape=jax.ShapeDtypeStruct((C, PR * 16, 128), jnp.bfloat16),
        in_specs=[
            pl.BlockSpec(memory_space=pltpu.SMEM),
            pl.BlockSpec(memory_space=pltpu.SMEM),
            pl.BlockSpec(memory_space=pltpu.VMEM),
            pl.BlockSpec(memory_space=pltpu.VMEM),
            pl.BlockSpec(memory_space=pltpu.VMEM),
            pl.BlockSpec(memory_space=pltpu.VMEM),
        ],
        out_specs=pl.BlockSpec(memory_space=pl.ANY),
        scratch_shapes=[
            pltpu.VMEM((WR // 2, 256, 128), jnp.float32),
            pltpu.VMEM((WR * C, 256), jnp.bfloat16),
            pltpu.VMEM((3, WR, 16, C, 128), jnp.bfloat16),
            pltpu.VMEM((WR * C, 128), jnp.bfloat16),
            pltpu.VMEM((C, 8, 128), jnp.float32),
            pltpu.VMEM((C, PR * 16, 128), jnp.bfloat16),
            pltpu.SemaphoreType.DMA((PR,)),
        ],
        compiler_params=pltpu.CompilerParams(vmem_limit_bytes=40 << 20),
        name="fine",
    )(where, bias_order, land, incoming, spread, taps)


def spread_of(interp):
    cells = interp.reshape(8, 2, 16, 16).transpose(2, 1, 0, 3)
    wide = jnp.tile(cells, (1, 1, 1, PC))
    same = jnp.arange(128)[None, :] // 16 + 1 == jnp.arange(WC)[:, None]
    inner = jnp.where(same[None, None, :, None, :], wide[:, :, None], 0)
    edges = jnp.stack([cells[..., 0], cells[..., 15]], axis=1).reshape(32, 2, 8).transpose(1, 2, 0)
    edges = jnp.pad(edges, ((0, 0), (0, 0), (0, 96)))
    column = jnp.where(jnp.arange(128) % 2 == 0, WC - 1, 0)
    same = column[None, :] == jnp.arange(WC)[:, None]
    outer = jnp.where(same[None, :, None, :], edges[:, None], 0)
    full = jnp.concatenate([inner, outer[None]], axis=0)
    return full.reshape(17, CELLS * WC, 128).astype(jnp.bfloat16)


def taps_of(kernel):
    by = kernel.transpose(2, 1, 0, 3)
    rows = jnp.stack([jnp.pad(by, ((0, 0), (0, 0), (r, 1 - r), (0, 0))) for r in range(2)], axis=1)
    rows = rows.reshape(C // 4, 4, 2, 12 * C)
    return jnp.stack([jnp.roll(rows, k, axis=1) for k in range(4)]).reshape(4, 2 * C, 12 * C)


def per_device(coarse, w_mix, interp, kernel, bias, block_ids, valid):
    n_lat, n_lon = 8, 16
    i = lax.axis_index("lat")
    j = lax.axis_index("lon")
    far = (pltpu.with_memory_space_constraint(v, pltpu.HBM) for v in (block_ids.T, coarse.reshape(CB_ROWS, CB_COLS, CELLS * C_IN), w_mix.T))
    outgoing = pack(*far)
    incoming = lax.all_to_all(outgoing, ("lat", "lon"), split_axis=0, concat_axis=0, tiled=True)
    first = block_ids[0, 0]
    owner = first // (CB_ROWS * CB_COLS)
    local = first % (CB_ROWS * CB_COLS)
    r0 = (local // CB_COLS) * n_lat + owner // n_lon
    c0 = (local % CB_COLS) * n_lon + owner % n_lon
    grid = valid.reshape(n_lat, n_lon, PR, PC).transpose(0, 2, 1, 3).reshape(n_lat * PR, n_lon * PC)
    window = lax.dynamic_slice(jnp.pad(grid, 1), (i * PR, j * PC), (WR, WC))
    row = jnp.arange(WR)[:, None]
    col = jnp.arange(WC)[None, :]
    source = (r0 + PR * i - 1 + row + 8) % n_lat * n_lon + (c0 + PC * j - 1 + col + 16) % n_lon
    where = jnp.where(window > 0, source * MOST + row // 8, -1).reshape(WR * WC).astype(jnp.int32)
    own = window[1:-1, 1:-1].astype(jnp.float32)
    land = jnp.repeat(own, 16, axis=1)
    bias_order = bias.reshape(C // 4, 4).T.reshape(C)
    near = (land, incoming, spread_of(interp), taps_of(kernel))
    near = tuple(pltpu.with_memory_space_constraint(v, pltpu.VMEM) for v in near)
    return fine(where, bias_order, *near)


def solution(mesh):
    placed = (P(("lat", "lon"), None), P(), P(), P(), P(), P(), P())
    return jax.shard_map(
        per_device, mesh=mesh, in_specs=placed, out_specs=P(None, "lat", "lon"), check_vma=False
    )
```
